32 devices in a mesh: dp: 8 (over z, y), head: 4 (over x, core).
Axes of the slice: x: 2, y: 2, z: 4, core: 2. Of those that a mesh axis runs over, the one named last changes fastest.
Arguments:
- q_latent: bfloat16 [1024, 1536], P('dp'), may hold values from -1000 to 1000
- kv_latent: bfloat16 [1024, 576], P('dp'), may hold values from -6 to 6
- kv_gain: float32 [512], replicated, may hold values from 0.1 to 1.9
- w_q_b: bfloat16 [1536, 12288], P(None, 'head'), may hold values from -0.15625 to 0.15625
- w_kv_b: bfloat16 [512, 16384], P(None, 'head'), may hold values from -0.25 to 0.25
- w_o: bfloat16 [8192, 7168], P('head', 'dp'), may hold values from -0.375 to 0.375
- prompt_len: int32 [1], replicated, may hold values from 1 to 255
- response_mask: int32 [1024], replicated, may hold values 0 or 1
Outputs:
- mixed: bfloat16 [1024, 7168], P('dp', 'head')
The draws below stay inside these ranges and needn't reach their ends.
All inputs are finite; a program needn't handle non-finite values.
Results may differ from the reference program's by a relative error of at most 0.013.
The reference program's roundings to bfloat16 on the way (of `keys`, `queries`, `query_rope`, `absorbed`, `weights`, `context` and `attended`) count: a program that leaves them out, or rounds other values in their place, can miss the bound.
Values may be sent and summed in bfloat16 or wider, within the bound.
A program may use at most 192 MiB of HBM per device.

```python
import math
import jax
import jax.numpy as jnp
from jax import lax

D = 7168
HEADS = 64
QR = 1536
KVR = 512
ROPE = 64
NOPE = 128
VD = 128
TOKENS = 1024


def draw_q_latent(key, part):
    values = jax.random.truncated_normal(jax.random.fold_in(key, 11), -3.0, 3.0, (TOKENS, QR), jnp.float32) * 2.0
    return values.astype(jnp.bfloat16)


def plant(array, own_key, low, largest):
    longest = array.shape.index(max(array.shape))
    spots = []
    for shift in (0, 1):
        where = [jax.random.randint(jax.random.fold_in(own_key, axis), (), 0, length) for axis, length in enumerate(array.shape)]
        where[longest] = (where[longest] + shift) % array.shape[longest]
        spots.append(tuple(where))
    return array.at[spots[0]].set(low).at[spots[1]].set(largest)


def raised(drawn, own_key, source, target, blocks, factor):
    def block_of(position):
        return (jnp.arange(drawn.shape[position]) // (drawn.shape[position] // blocks)).reshape((-1,) + (1,) * (drawn.ndim - 1 - position))

    one_side = jax.random.permutation(own_key, blocks)[block_of(target)]
    far = (block_of(target) + blocks // 2) % blocks
    return jnp.where((block_of(source) == one_side) | (block_of(source) == far), factor * drawn, drawn)


def shard_levels(key, shape, cuts, low, high):
    def one(axis_at, blocks):
        draws = jax.random.uniform(jax.random.fold_in(jax.random.fold_in(key, 6), axis_at), (blocks,), jnp.float32, low / len(cuts), high / len(cuts))
        return jnp.repeat(jnp.exp(draws), shape[axis_at] // blocks).reshape((-1,) + (1,) * (len(shape) - axis_at - 1))

    loudness = one(*cuts[0])
    for cut in cuts[1:]:
        loudness = loudness * one(*cut)
    return loudness


def bell_draw(key, shape, spread, reach, split=(), kind=jnp.bfloat16):
    level = shard_levels(key, shape, split, -0.22, 0.18) if split else 1.0
    values = jax.random.normal(key, shape, jnp.float32) * spread * level
    return jnp.minimum(jnp.maximum(values, -reach), reach).astype(kind)


def noise_with(stream_key, shape, width, limit, split, heavy, kind=jnp.bfloat16):
    array = width * jax.random.normal(stream_key, shape, jnp.float32)
    if split:
        array = array * shard_levels(stream_key, shape, split, -0.22, 0.18)
    return jnp.clip(raised(array, jax.random.fold_in(stream_key, 3), *heavy), -limit, limit).astype(kind)


def setup_inputs(seed: int = 0) -> dict:
    seeds = jax.random.split(jax.random.key(seed), 9)
    return {
        "q_latent": draw_q_latent(jax.random.fold_in(seeds[8], 71), 0),
        "kv_latent": bell_draw(seeds[1], (TOKENS, KVR + ROPE), 1.0, 6.0, ((0, 8),)),
        "kv_gain": jnp.clip(1.0 + 0.18 * jax.random.normal(seeds[2], (KVR,), jnp.float32), 0.1, 1.9),
        "w_q_b": bell_draw(seeds[3], (QR, HEADS * (NOPE + ROPE)), QR ** -0.5, 0.15625, ((1, 4),)),
        "w_kv_b": bell_draw(seeds[4], (KVR, HEADS * (NOPE + VD)), KVR ** -0.5, 0.25, ((1, 4),)),
        "w_o": noise_with(seeds[5], (HEADS * VD, D), (VD * 4) ** -0.5, 0.375, ((0, 4), (1, 8)), (0, 1, 8, 2.0)),
        "prompt_len": jax.random.randint(seeds[6], (1,), 1, TOKENS // 4).astype(jnp.int32),
        "response_mask": plant((jax.random.randint(seeds[7], (TOKENS,), 0, 2) < 1).astype(jnp.int32), jax.random.fold_in(seeds[7], 1), 0, 1),
    }


epsilon = 1e-06

def tables(positions):
    half_width = ROPE // 2
    frequency = 10000.0 ** (-jnp.arange(half_width, dtype=jnp.float32) * 2.0 / ROPE)
    angles = positions.astype(jnp.float32)[:, None] * frequency[None, :]
    return (jnp.cos(angles), jnp.sin(angles))

def rotate(values, cosine, sine_table):
    half_width = values.shape[-1] // 2
    leading = values[..., :half_width]
    trailing = values[..., half_width:]
    return jnp.concatenate([leading * cosine - trailing * sine_table, trailing * cosine + leading * sine_table], axis=-1)

def reference(q_latent, kv_latent, kv_gain, w_q_b, w_kv_b, w_o, prompt_len, response_mask):
    positions = jnp.arange(TOKENS, dtype=jnp.int32)
    cosine, sine_table = tables(positions)
    latent = kv_latent[:, :KVR].astype(jnp.float32)
    normed = latent * lax.rsqrt(lax.optimization_barrier(jnp.mean(latent * latent, axis=-1, keepdims=True)) + epsilon) * kv_gain
    key_rope = rotate(kv_latent[:, KVR:].astype(jnp.float32), cosine, sine_table)
    keys = jnp.concatenate([normed, key_rope], axis=1).astype(jnp.bfloat16)
    queries = jnp.dot(q_latent, w_q_b, preferred_element_type=jnp.float32).astype(jnp.bfloat16)
    queries = queries.reshape(TOKENS, HEADS, NOPE + ROPE)
    query_rope = rotate(queries[:, :, NOPE:].astype(jnp.float32), cosine[:, None, :], sine_table[:, None, :]).astype(jnp.bfloat16)
    w_heads = w_kv_b.reshape(KVR, HEADS, NOPE + VD)
    absorbed = jnp.einsum('thn,khn->thk', queries[:, :, :NOPE].astype(jnp.float32), w_heads[:, :, :NOPE].astype(jnp.float32)).astype(jnp.bfloat16)
    full_query = jnp.concatenate([absorbed, query_rope], axis=-1)
    usable = (positions < prompt_len[0]) | (response_mask == 1)
    allowed = (positions[None, :] <= positions[:, None]) & usable[None, :]
    keys_wide = keys.astype(jnp.float32)
    latent_values = keys_wide[:, :KVR]
    scale = 1.0 / math.sqrt(NOPE + ROPE)
    group_size = math.gcd(HEADS, 4)
    groups = HEADS // group_size
    grouped = full_query.reshape(TOKENS, groups, group_size, KVR + ROPE).transpose(1, 0, 2, 3)
    value_blocks = w_heads[:, :, NOPE:].reshape(KVR, groups, group_size, VD).transpose(1, 0, 2, 3)

    def one_group(operands):
        chosen, w_group = operands
        scores = jnp.einsum('tgc,sc->tgs', chosen.astype(jnp.float32), keys_wide) * scale
        scores = jnp.where(allowed[:, None, :], scores, -1e+30)
        row_max = lax.optimization_barrier(jnp.max(scores, axis=-1, keepdims=True))
        lifted = jnp.exp(scores - row_max)
        weights = (lifted / lax.optimization_barrier(jnp.sum(lifted, axis=-1, keepdims=True))).astype(jnp.bfloat16)
        context = jnp.einsum('tgs,sc->tgc', weights.astype(jnp.float32), latent_values).astype(jnp.bfloat16)
        return jnp.einsum('tgc,cgv->tgv', context.astype(jnp.float32), w_group.astype(jnp.float32)).astype(jnp.bfloat16)
    outputs = lax.map(one_group, (grouped, value_blocks))
    attended = outputs.transpose(1, 0, 2, 3).reshape(TOKENS, HEADS * VD)
    return jnp.dot(attended, w_o, preferred_element_type=jnp.float32).astype(jnp.bfloat16)
```

```python
import functools
import math

import jax
import jax.numpy as jnp
from jax import lax
from jax.experimental import pallas as pl
from jax.experimental.pallas import tpu as pltpu
from jax.sharding import PartitionSpec as P

KVR = 512
ROPE = 64
NOPE = 128
VD = 128


epsilon = 1e-06


def tables(positions):
    half_width = ROPE // 2
    frequency = 10000.0 ** (-jnp.arange(half_width, dtype=jnp.float32) * 2.0 / ROPE)
    angles = positions.astype(jnp.float32)[:, None] * frequency[None, :]
    return (jnp.cos(angles), jnp.sin(angles))


def rotate(values, cosine, sine_table):
    half_width = values.shape[-1] // 2
    leading = values[..., :half_width]
    trailing = values[..., half_width:]
    return jnp.concatenate(
        [leading * cosine - trailing * sine_table, trailing * cosine + leading * sine_table],
        axis=-1,
    )


def attend(full_query, keys, allowed, w_value):
    rows_here, head_count = (full_query.shape[0], full_query.shape[1])
    group_size = math.gcd(head_count, 4)
    groups = head_count // group_size
    grouped = full_query.reshape(rows_here, groups, group_size, KVR + ROPE).transpose(1, 0, 2, 3)
    value_blocks = w_value.reshape(KVR, groups, group_size, VD).transpose(1, 0, 2, 3)
    latent_values = keys[:, :KVR]
    scale = 1.0 / math.sqrt(NOPE + ROPE)

    def one_group(operands):
        chosen, w_group = operands
        scores = jnp.einsum("tgc,sc->tgs", chosen, keys, preferred_element_type=jnp.float32) * scale
        scores = jnp.where(allowed[:, None, :], scores, -1e30)
        row_max = jnp.max(scores, axis=-1, keepdims=True)
        lifted = jnp.exp(scores - row_max)
        weights = (lifted / jnp.sum(lifted, axis=-1, keepdims=True)).astype(jnp.bfloat16)
        context = jnp.einsum(
            "tgs,sc->tgc", weights, latent_values, preferred_element_type=jnp.float32
        ).astype(jnp.bfloat16)
        return jnp.einsum(
            "tgc,cgv->tgv", context, w_group, preferred_element_type=jnp.float32
        ).astype(jnp.bfloat16)

    outputs = lax.map(one_group, (grouped, value_blocks))
    return outputs.transpose(1, 0, 2, 3).reshape(rows_here, head_count * VD)


def local(q_latent, kv_latent, kv_gain, w_q_b, w_kv_b, w_o, prompt_len, response_mask):
    rows_here = q_latent.shape[0]
    offset = lax.axis_index("dp") * rows_here
    local_positions = offset + jnp.arange(rows_here, dtype=jnp.int32)
    cosine, sine_table = tables(local_positions)
    latent = kv_latent[:, :KVR].astype(jnp.float32)
    normed = (
        latent * lax.rsqrt(jnp.mean(latent * latent, axis=-1, keepdims=True) + epsilon) * kv_gain
    )
    key_rope = rotate(kv_latent[:, KVR:].astype(jnp.float32), cosine, sine_table)
    local_keys = jnp.concatenate([normed, key_rope], axis=1).astype(jnp.bfloat16)
    keys = lax.all_gather(local_keys, "dp", axis=0, tiled=True)
    head_count = w_q_b.shape[1] // (NOPE + ROPE)
    queries = jnp.dot(q_latent, w_q_b, preferred_element_type=jnp.float32).astype(jnp.bfloat16)
    queries = queries.reshape(rows_here, head_count, NOPE + ROPE)
    query_rope = rotate(
        queries[:, :, NOPE:].astype(jnp.float32), cosine[:, None, :], sine_table[:, None, :]
    ).astype(jnp.bfloat16)
    w_heads = w_kv_b.reshape(KVR, head_count, NOPE + VD)
    absorbed = jnp.einsum(
        "thn,khn->thk",
        queries[:, :, :NOPE],
        w_heads[:, :, :NOPE],
        preferred_element_type=jnp.float32,
    ).astype(jnp.bfloat16)
    full_query = jnp.concatenate([absorbed, query_rope], axis=-1)
    key_positions = jnp.arange(keys.shape[0], dtype=jnp.int32)
    usable = (key_positions < prompt_len[0]) | (response_mask == 1)
    allowed = (key_positions[None, :] <= local_positions[:, None]) & usable[None, :]
    attended = attend(full_query, keys, allowed, w_heads[:, :, NOPE:])
    spread = jnp.dot(
        lax.all_gather(attended, "dp", axis=0, tiled=True), w_o, preferred_element_type=jnp.float32
    )
    partial_value = lax.all_to_all(spread, "dp", split_axis=0, concat_axis=1, tiled=True)
    return lax.psum_scatter(partial_value, "head", scatter_dimension=1, tiled=True).astype(
        jnp.bfloat16
    )


MESH = pl.DeviceIdType.MESH
LOG2E = 1.4426950408889634
QB = 256


def gather_kernel(n, x_ref, out_ref, own_sem, send_sem, recv_sem, psend_sem, precv_sem):
    me = lax.axis_index("dp")
    g = lax.axis_index("head")
    half = n // 2
    rows = x_ref.shape[0]
    part = rows // 2
    core = lax.rem(g, 2)
    mate = g + 1 - 2 * core
    start = core * part

    def place(j):
        return lax.rem(j, 2) * (n - 1 - j // 2) + (1 - lax.rem(j, 2)) * (j // 2)

    def owner(p):
        upper = p // half
        return (1 - upper) * (2 * p) + upper * (2 * (n - 1 - p) + 1)

    here = place(me)
    right = owner(lax.rem(here + 1, n))
    left = owner(lax.rem(here + n - 1, n))

    barrier = pltpu.get_barrier_semaphore()
    pl.semaphore_signal(barrier, inc=1, device_id=(left, g), device_id_type=MESH)
    pl.semaphore_signal(barrier, inc=1, device_id=(right, g), device_id_type=MESH)
    pl.semaphore_signal(barrier, inc=1, device_id=(me, mate), device_id_type=MESH)
    pl.semaphore_wait(barrier, 3)

    own = pltpu.make_async_copy(x_ref, out_ref.at[me], own_sem)
    own.start()

    def span(step, way):
        if step < half - 1:
            return start, part
        return start + way * (part // 2), part // 2

    def ring(step, way, block, target):
        first, count = span(step, way)
        first = pl.multiple_of(first, count)
        if step == 0:
            source = x_ref.at[pl.ds(first, count)]
        else:
            source = out_ref.at[block, pl.ds(first, count)]
        return pltpu.make_async_remote_copy(
            src_ref=source,
            dst_ref=out_ref.at[block, pl.ds(first, count)],
            send_sem=send_sem.at[way, step],
            recv_sem=recv_sem.at[way, step],
            device_id=(target, g),
            device_id_type=MESH,
        )

    def share(step, way, block):
        first, count = span(step, way)
        first = pl.multiple_of(first, count)
        return pltpu.make_async_remote_copy(
            src_ref=out_ref.at[block, pl.ds(first, count)],
            dst_ref=out_ref.at[block, pl.ds(first, count)],
            send_sem=psend_sem.at[way, step],
            recv_sem=precv_sem.at[way, step],
            device_id=(me, mate),
            device_id_type=MESH,
        )

    rings, shares = [], []
    for step in range(half):
        right_copy = ring(step, 0, owner(lax.rem(here + n - step, n)), right)
        left_copy = ring(step, 1, owner(lax.rem(here + step, n)), left)
        right_copy.start()
        left_copy.start()
        rings += [right_copy, left_copy]
        right_copy.wait_recv()
        copy = share(step, 0, owner(lax.rem(here + n - step - 1, n)))
        copy.start()
        shares.append(copy)
        left_copy.wait_recv()
        copy = share(step, 1, owner(lax.rem(here + step + 1, n)))
        copy.start()
        shares.append(copy)
    own.wait()
    for copy in rings:
        copy.wait_send()
    for copy in shares:
        copy.wait()


def compute_kernel(
    x_hbm, wq_hbm, wkv_hbm, wo_hbm, gain_ref, cosk_ref, sink_ref, cq_ref, sa_ref, sb_ref, bias_ref,
    out_ref,
    x, wq, wkv, wo, keys, kslab, vbuf, att, mask, sems,
):
    tokens = x.shape[0]
    qr = wq.shape[0]
    pairs = wkv.shape[1] // (2 * (NOPE + VD))
    copies = [
        pltpu.make_async_copy(x_hbm, x, sems.at[0]),
        pltpu.make_async_copy(wkv_hbm, wkv, sems.at[1]),
        pltpu.make_async_copy(wq_hbm, wq, sems.at[2]),
        pltpu.make_async_copy(wo_hbm, wo, sems.at[3]),
    ]
    for copy in copies:
        copy.start()
    copies[0].wait()
    scale = LOG2E / math.sqrt(NOPE + ROPE)

    latent = x[:, qr : qr + KVR].astype(jnp.float32)
    mean = jnp.mean(latent * latent, axis=-1, keepdims=True)
    keys[...] = (latent * lax.rsqrt(mean + epsilon) * gain_ref[...]).astype(jnp.bfloat16)
    rope = x[:, qr + KVR :].astype(jnp.float32)
    half = ROPE // 2
    turned = jnp.concatenate([-rope[:, half:], rope[:, :half]], axis=1)
    key_rope = (rope * cosk_ref[...] + turned * sink_ref[...]).astype(jnp.bfloat16)
    blank = jnp.zeros((tokens, NOPE - ROPE), jnp.bfloat16)
    even_tail = jnp.concatenate([key_rope, blank], axis=1)
    for p in range(pairs):
        kslab[p, :, 128:256] = even_tail
    copies[1].wait()

    @pl.loop(0, pairs)
    def _(p):
        width = 2 * (NOPE + VD)
        w = wkv[:, pl.ds(pl.multiple_of(p * width, width), width)]
        for r in range(tokens // QB):
            rows = slice(r * QB, (r + 1) * QB)
            both = jnp.dot(keys[rows, :], w, preferred_element_type=jnp.float32).astype(jnp.bfloat16)
            kslab[p, rows, 0:128] = both[:, 0:128]
            vbuf[p, rows, 0:128] = both[:, 128:256]
            vbuf[p, rows, 128:256] = both[:, 384:512]
            odd = both[:, 256:384]
            kslab[p, rows, 256:384] = jnp.concatenate([blank[rows], odd[:, :64]], axis=1)
            kslab[p, rows, 384:512] = jnp.concatenate([odd[:, 64:], kslab[p, rows, 128:192]], axis=1)

    copies[2].wait()
    for r in range(tokens // QB):
        rows = slice(r * QB, (r + 1) * QB)
        end = (r + 1) * QB
        row_ids = r * QB + lax.broadcasted_iota(jnp.int32, (QB, end), 0)
        col_ids = lax.broadcasted_iota(jnp.int32, (QB, end), 1)
        mask[:, :end] = jnp.where(col_ids <= row_ids, bias_ref[:, :end], -1e30)

        @pl.loop(0, pairs)
        def _(p):
            w = wq[:, pl.ds(pl.multiple_of(p * 384, 384), 384)]
            q = jnp.dot(x[rows, :qr], w, preferred_element_type=jnp.float32).astype(jnp.bfloat16)
            v = q[:, 128:384].astype(jnp.float32)
            v = (
                v * cq_ref[rows, :]
                + pltpu.roll(v, 256 - half, 1) * sa_ref[rows, :]
                + pltpu.roll(v, half, 1) * sb_ref[rows, :]
            ).astype(jnp.bfloat16)
            slabs = (jnp.concatenate([q[:, :128], v[:, :128]], axis=1), v)
            for h in range(2):
                s = lax.dot_general(
                    slabs[h], kslab[p, :end, 256 * h : 256 * h + 256],
                    (((1,), (1,)), ((), ())), preferred_element_type=jnp.float32,
                )
                s = s * scale + mask[:, :end]
                top = jnp.max(s, axis=-1, keepdims=True)
                e = jnp.exp2(s - top)
                total = jnp.sum(e, axis=-1, keepdims=True)
                o = jnp.dot(
                    e.astype(jnp.bfloat16), vbuf[p, :end, 128 * h : 128 * h + 128],
                    preferred_element_type=jnp.float32,
                )
                at = pl.ds(pl.multiple_of(p * 256 + 128 * h, 128), 128)
                att[:, at] = (o / total).astype(jnp.bfloat16)

        if r == 0:
            copies[3].wait()
        out_ref[rows, :] = jnp.dot(att[...], wo[...], preferred_element_type=jnp.float32).astype(jnp.bfloat16)


def reduce_kernel(n, heads, part_ref, out_ref, from_mate, summed, arrived, msend, mrecv, send_sem, recv_sem):
    me = lax.axis_index("dp")
    g = lax.axis_index("head")
    core = lax.rem(g, 2)
    mate = g + 1 - 2 * core
    side = g // 2
    sides = heads // 2
    per = n // heads
    target = me // per
    slot = lax.rem(me, per) * sides + side
    cols = part_ref.shape[2]

    first = []
    for k in range(n // 2):
        copy = pltpu.make_async_remote_copy(
            src_ref=part_ref.at[2 * k + 1 - core],
            dst_ref=from_mate.at[k],
            send_sem=msend.at[k],
            recv_sem=mrecv.at[k],
            device_id=(me, mate),
            device_id_type=MESH,
        )
        copy.start()
        first.append(copy)

    def second(k):
        return pltpu.make_async_remote_copy(
            src_ref=summed.at[k],
            dst_ref=arrived.at[slot],
            send_sem=send_sem.at[k],
            recv_sem=recv_sem.at[slot],
            device_id=(2 * k + core, target),
            device_id_type=MESH,
        )

    for k in range(n // 2):
        first[k].wait_recv()
        summed[k] = (
            part_ref[2 * k + core].astype(jnp.float32) + from_mate[k].astype(jnp.float32)
        ).astype(jnp.bfloat16)
        mine = (2 * k + core == me) & (target == g)

        @pl.when(mine)
        def _():
            arrived[slot] = summed[k]

        @pl.when(jnp.logical_not(mine))
        def _():
            second(k).start()

    for a in range(per):
        for b in range(sides):
            source = g * per + a
            mine = (source == me) & (lax.rem(me, 2) == core) & (b == side)

            @pl.when(jnp.logical_not(mine))
            def _():
                pltpu.make_async_remote_copy(
                    src_ref=summed.at[0],
                    dst_ref=arrived.at[a * sides + b],
                    send_sem=send_sem.at[0],
                    recv_sem=recv_sem.at[a * sides + b],
                    device_id=(source, g),
                    device_id_type=MESH,
                ).wait_recv()

        total = arrived[a * sides].astype(jnp.float32)
        for b in range(1, sides):
            total = total + arrived[a * sides + b].astype(jnp.float32)
        out_ref[:, a * cols : (a + 1) * cols] = total.astype(jnp.bfloat16)

    for k in range(n // 2):
        mine = (2 * k + core == me) & (target == g)

        @pl.when(jnp.logical_not(mine))
        def _():
            second(k).wait_send()

        first[k].wait_send()


ANY = pl.BlockSpec(memory_space=pl.ANY)
VMEM = pl.BlockSpec(memory_space=pltpu.VMEM)


def fused(n, heads, q_latent, kv_latent, kv_gain, w_q_b, w_kv_b, w_o, prompt_len, response_mask):
    rows, qr = q_latent.shape
    tokens = rows * n
    width = qr + KVR + ROPE
    cols = w_o.shape[1]
    pairs = w_kv_b.shape[1] // (2 * (NOPE + VD))
    x = jnp.concatenate([q_latent, kv_latent], axis=1)
    steps = n // 2
    gathered = pl.pallas_call(
        functools.partial(gather_kernel, n),
        out_shape=jax.ShapeDtypeStruct((n, rows, width), jnp.bfloat16),
        in_specs=[VMEM],
        out_specs=ANY,
        scratch_shapes=[pltpu.SemaphoreType.DMA] + [pltpu.SemaphoreType.DMA((2, steps))] * 4,
        compiler_params=pltpu.CompilerParams(collective_id=0, has_side_effects=True),
        name="gather_rows",
    )(x).reshape(tokens, width)

    positions = jnp.arange(tokens, dtype=jnp.int32)
    cosine, sine_table = tables(positions)
    one = jnp.ones((tokens, NOPE), jnp.float32)
    none = jnp.zeros((tokens, NOPE), jnp.float32)
    zero = jnp.zeros_like(sine_table)
    cosk = jnp.concatenate([cosine, cosine], axis=1)
    sink = jnp.concatenate([sine_table, sine_table], axis=1)
    cq = jnp.concatenate([cosk, one, cosk], axis=1)
    sa = jnp.concatenate([-sine_table, zero, none, -sine_table, zero], axis=1)
    sb = jnp.concatenate([zero, sine_table, none, zero, sine_table], axis=1)
    usable = (positions < prompt_len[0]) | (response_mask == 1)
    bias = jnp.where(usable, 0.0, -1e30).astype(jnp.float32)[None, :]
    bf = jnp.bfloat16
    partial_sum = pl.pallas_call(
        compute_kernel,
        out_shape=jax.ShapeDtypeStruct((tokens, cols), bf),
        in_specs=[ANY] * 4 + [VMEM] * 7,
        out_specs=VMEM,
        scratch_shapes=[
            pltpu.VMEM((tokens, width), bf),
            pltpu.VMEM(w_q_b.shape, bf),
            pltpu.VMEM(w_kv_b.shape, bf),
            pltpu.VMEM(w_o.shape, bf),
            pltpu.VMEM((tokens, KVR), bf),
            pltpu.VMEM((pairs, tokens, 512), bf),
            pltpu.VMEM((pairs, tokens, 2 * VD), bf),
            pltpu.VMEM((QB, 2 * pairs * VD), bf),
            pltpu.VMEM((QB, tokens), jnp.float32),
            pltpu.SemaphoreType.DMA((4,)),
        ],
        compiler_params=pltpu.CompilerParams(vmem_limit_bytes=60 * 1024 * 1024),
        name="attend_project",
    )(gathered, w_q_b, w_kv_b, w_o, kv_gain[None, :], cosk, sink, cq, sa, sb, bias)

    half = n // 2
    slots = (n // heads) * (heads // 2)
    return pl.pallas_call(
        functools.partial(reduce_kernel, n, heads),
        out_shape=jax.ShapeDtypeStruct((rows, cols * (n // heads)), bf),
        in_specs=[VMEM],
        out_specs=VMEM,
        scratch_shapes=[
            pltpu.VMEM((half, rows, cols), bf),
            pltpu.VMEM((half, rows, cols), bf),
            pltpu.VMEM((slots, rows, cols), bf),
            pltpu.SemaphoreType.DMA((half,)),
            pltpu.SemaphoreType.DMA((half,)),
            pltpu.SemaphoreType.DMA((half,)),
            pltpu.SemaphoreType.DMA((slots,)),
        ],
        compiler_params=pltpu.CompilerParams(has_side_effects=True),
        name="reduce_rows",
    )(partial_sum.reshape(n, rows, cols))


def solution(mesh):
    n, heads = mesh.shape["dp"], mesh.shape["head"]

    def step(*arrays):
        rows, cols = arrays[0].shape[0], arrays[5].shape[1]
        fits = rows * n <= 1024 and cols % 128 == 0 and n % heads == 0 and heads % 2 == 0
        return fused(n, heads, *arrays) if fits else local(*arrays)

    return jax.shard_map(
        step,
        mesh=mesh,
        in_specs=(
            P("dp", None),
            P("dp", None),
            P(),
            P(None, "head"),
            P(None, "head"),
            P("head", "dp"),
            P(),
            P(),
        ),
        out_specs=P("dp", "head"),
        check_vma=False,
    )
```
